16 devices in a mesh: rep: 1, dp: 16 (over x, y, z, core).
Axes of the slice: x: 2, y: 2, z: 2, core: 2. Of those that a mesh axis runs over, the one named last changes fastest.
Arguments:
- x: bfloat16 [16, 2048, 1024], P(('rep', 'dp'))
- dy: bfloat16 [16, 2048, 1024], P(('rep', 'dp'))
- w_gate: bfloat16 [2, 1024, 6144], P(None, 'dp')
- w_up: bfloat16 [2, 1024, 6144], P(None, 'dp')
- w_down: bfloat16 [2, 6144, 1024], P(None, 'dp')
Outputs:
- output 1: bfloat16 [16, 2048, 1024], P(('rep', 'dp'))
- output 2: bfloat16 [2, 1024, 6144], P('rep', 'dp')
- output 3: bfloat16 [2, 1024, 6144], P('rep', 'dp')
- output 4: bfloat16 [2, 6144, 1024], P('rep', 'dp')
All inputs are finite; a program needn't handle non-finite values.
Results may differ from the reference program's by a relative error of at most 0.018.
Values are sent between devices in bfloat16 or wider.
A program may use at most 2 GiB of HBM per device.

```python
import jax
import jax.numpy as jnp
from jax import lax

SEQUENCES = 16
TOKENS = 2048
D = 1024
FF = 6144
LAYERS = 2
NAMES = ("w_gate", "w_up", "w_down")
SHAPES = {"w_gate": (LAYERS, D, FF), "w_up": (LAYERS, D, FF), "w_down": (LAYERS, FF, D)}


def bump(key, n, height):
    away = (jnp.arange(n, dtype=jnp.int32) - jax.random.randint(key, (), 0, n, jnp.int32)) % n
    return jnp.where(away < n // 8, height, 1.0)


def together(key, own, strength):
    shared = jax.random.normal(key, own.shape[1:], jnp.float32)
    return (own + strength * shared) * lax.rsqrt(1 + strength * strength)


def setup_inputs(seed: int = 0, part: int = 0) -> dict:
    kx, kdy, ka, kb, kz, kf, kh, kl, *kw = jax.random.split(jax.random.key(seed), 8 + len(NAMES))
    kx, kdy, ka, kb = (jax.random.fold_in(k, part) for k in (kx, kdy, ka, kb))
    shape = (SEQUENCES, TOKENS, D)
    much_x, much_dy = jax.random.uniform(kz, (2,), jnp.float32, 0.0, 1.0)
    layers = 2.0 ** jax.random.uniform(kl, (LAYERS, 1, 1), jnp.float32, -1.0, 1.0)
    x = together(ka, jax.random.normal(kx, shape, jnp.float32), much_x) * bump(kf, D, 4.0)
    dy = together(kb, jax.random.normal(kdy, shape, jnp.float32), much_dy)
    drawn = {"x": x.astype(jnp.bfloat16), "dy": (dy * (SEQUENCES * TOKENS) ** -0.5).astype(jnp.bfloat16)}
    for key, name in zip(kw, NAMES, strict=True):
        w = jax.random.normal(key, SHAPES[name], jnp.float32) * SHAPES[name][1] ** -0.5
        drawn[name] = (w * {"w_gate": 1.0, "w_up": bump(kh, FF, 4.0), "w_down": layers}[name]).astype(jnp.bfloat16)
    return drawn


def matmul(a, w):
    return jnp.dot(a, w, preferred_element_type=jnp.float32).astype(jnp.bfloat16)


def normed(h):
    wide = h.astype(jnp.float32)
    scale = lax.rsqrt(jnp.mean(wide**2, -1, keepdims=True) + 1e-6)
    return (wide * scale).astype(jnp.bfloat16)


def layer(h, w):
    a = normed(h)
    gate = jnp.dot(a, w["w_gate"], preferred_element_type=jnp.float32)
    up = jnp.dot(a, w["w_up"], preferred_element_type=jnp.float32)
    return h + matmul((jax.nn.silu(gate) * up).astype(jnp.bfloat16), w["w_down"])


def stack(weights, h):
    return lax.scan(lambda h, w: (layer(h, w), None), h, weights)[0]


def reference(x, dy, w_gate, w_up, w_down):
    weights = dict(zip(NAMES, (w_gate, w_up, w_down), strict=True))

    def take(so_far, sequence):
        h, by_y = sequence
        _, back = jax.vjp(stack, weights, h)
        by_weights, by_h = back(by_y)
        return jax.tree.map(lambda total, term: total + term.astype(jnp.float32), so_far, by_weights), by_h

    none_yet = {name: jnp.zeros(w.shape, jnp.float32) for name, w in weights.items()}
    by_weights, by_x = lax.scan(take, none_yet, (x, dy))
    return (by_x, *(by_weights[name].astype(jnp.bfloat16) for name in NAMES))
```

```python
import jax
import jax.numpy as jnp
from jax import lax
from jax.sharding import PartitionSpec as P

LAYERS = 2
BF, F32 = jnp.bfloat16, jnp.float32


def dot(a, b, dims):
    return lax.dot_general(a, b, (dims, ((), ())), preferred_element_type=F32)


NN, NT, TN = ((1,), (0,)), ((1,), (1,)), ((0,), (0,))


def scale_of(h):
    wide = h.astype(F32)
    return lax.rsqrt(jnp.mean(wide**2, -1, keepdims=True) + 1e-6)


def norm_back(h, scale, da):
    wide = h.astype(F32)
    inner = jnp.mean(wide * da, -1, keepdims=True)
    return scale * da - wide * (scale**3 * inner)


def solution(mesh):
    def body(x, dy, w_gate, w_up, w_down):
        x, dy = x[0], dy[0]
        gather = lambda w: lax.all_gather(w, "dp", axis=0, tiled=True)
        scatter = lambda g: lax.psum_scatter(g, "dp", scatter_dimension=0, tiled=True)
        wg, wu, wd = ([gather(w[n]) for n in range(LAYERS)] for w in (w_gate, w_up, w_down))
        h, kept = x, []
        for n in range(LAYERS):
            scale = scale_of(h)
            a = (h.astype(F32) * scale).astype(BF)
            gate, up = dot(a, wg[n], NN), dot(a, wu[n], NN)
            hid = (jax.nn.silu(gate) * up).astype(BF)
            kept.append((h, scale, a, gate, up, hid))
            if n < LAYERS - 1:
                h = h + dot(hid, wd[n], NN).astype(BF)
        dh, grads = dy, [None] * LAYERS
        for n in reversed(range(LAYERS)):
            h, scale, a, gate, up, hid = kept[n]
            dwd = scatter(dot(hid, dh, TN).astype(BF))
            dhid = dot(dh, wd[n], NT).astype(BF).astype(F32)
            sig = jax.nn.sigmoid(gate)
            silu = gate * sig
            dgate = (dhid * up * (sig + silu * (1 - sig))).astype(BF)
            dup = (dhid * silu).astype(BF)
            dwg = scatter(dot(a, dgate, TN).astype(BF))
            dwu = scatter(dot(a, dup, TN).astype(BF))
            da = dot(dgate, wg[n], NT) + dot(dup, wu[n], NT)
            dh = (dh.astype(F32) + norm_back(h, scale, da)).astype(BF)
            grads[n] = (dwg, dwu, dwd)
        return (dh[None], *(jnp.stack([g[k] for g in grads]) for k in range(3)))

    rows = P(None, "dp", None)
    data = P(("rep", "dp"), None, None)
    return jax.shard_map(body, mesh=mesh, in_specs=(data, data, rows, rows, rows), out_specs=(data, rows, rows, rows), check_vma=False)
```

```python
import functools

import jax
import jax.numpy as jnp
from jax import lax
from jax.experimental import pallas as pl
from jax.experimental.pallas import tpu as pltpu
from jax.sharding import PartitionSpec as P

BF, F32 = jnp.bfloat16, jnp.float32
MESH = pl.DeviceIdType.MESH
R = 128
D = CW = 8 * R
TT = 256
HT, NT = 8, 16
TB, BT = 2 * TT, NT // 2
T = HT * TT
U = 3
VMEM_LIMIT = 67_043_328

M = 3
ITEMS = [f"{m}0{j}" for j in range(U) for m in "gu"] + [f"d0{j}" for j in range(U)] + [f"{m}1{j}" for j in range(U) for m in "gud"]
NI = len(ITEMS)
PLANES = range(3)
LAST = (HT - 2, HT - 1)
NN, NTR, TN = ((1,), (0,)), ((1,), (1,)), ((0,), (0,))


def triple(n):
    return range(3 * n, 3 * n + 3)


def odd(t):
    return lax.rem(t, 2)


def dot(a, b, dims):
    return lax.dot_general(a, b, (dims, ((), ())), preferred_element_type=F32)


def scale_of(wide):
    return lax.rsqrt(jnp.mean(wide**2, -1, keepdims=True) + 1e-6)


def cols(k, parts=4):
    return slice(k * CW // parts, (k + 1) * CW // parts)


class Place:
    def __init__(self):
        me = lax.axis_index("dp")
        self.c = odd(me)
        p = me // 2
        self.b = [lax.rem(p // 4, 2), lax.rem(p // 2, 2), odd(p)]
        self.partner = (0, me + 1 - 2 * self.c)

    def chip(self, flips):
        b = [1 - v if f else v for v, f in zip(self.b, flips, strict=True)]
        return b[0] * 4 + b[1] * 2 + b[2]

    def neighbour(self, dim):
        return (0, self.chip([dim == d for d in PLANES]) * 2 + self.c)

    def rows(self, q, k):
        flips = [0, 0, 0]
        for j in PLANES:
            flips[(k + j) % 3] = (q >> (2 - j)) & 1
        return pl.ds(pl.multiple_of(self.chip(flips) * R, R), R)

    def greet(self):
        bar = pltpu.get_barrier_semaphore()
        for device in (*map(self.neighbour, PLANES), self.partner):
            pl.semaphore_signal(bar, inc=1, device_id=device, device_id_type=MESH)
        pl.semaphore_wait(bar, 4)


def copy(src, dst, sem):
    return pltpu.make_async_copy(src, dst, sem)


def remote(src, dst, send, recv, device):
    return pltpu.make_async_remote_copy(src, dst, send, recv, device_id=device, device_id_type=MESH)


def arrived(ref, sem):
    copy(ref, ref, sem).wait()


def tile(t, size=None):
    size = size or TT
    return pl.ds(pl.multiple_of(t * size, size), size)


def lanes(p, parity, u):
    return pl.ds(pl.multiple_of(((2 * p + parity) * U + u) * R, R), R)


def each(n, f):
    def body(p, carry):
        f(p)
        return carry

    lax.fori_loop(0, n, body, 0)


class Gather:
    def __init__(self, at, st, w, ssem, rsem):
        self.at, self.st, self.w, self.ssem, self.rsem = at, st, w, ssem, rsem

    def send(self, i, q, j):
        k = i % 3
        rows = self.at.rows(q, k)
        src = self.st.at[i] if q == 0 else self.w.at[i, rows]
        remote(src, self.w.at[i, rows], self.ssem.at[i], self.rsem.at[i, (q | (4 >> j)) - 1], self.at.neighbour((k + j) % 3)).start()

    def wait(self, i, q):
        arrived(self.w.at[i, self.at.rows(q, i % 3)], self.rsem.at[i, q - 1])

    def s0(self, n):
        for j in PLANES:
            for i in triple(n):
                self.send(i, 0, j)

    def s1(self, n):
        with jax.named_scope(f"s1#n={n}"):
            for i in triple(n):
                self.wait(i, 4)
            for j in (1, 2):
                for i in triple(n):
                    self.send(i, 4, j)

    def s2(self, n):
        with jax.named_scope(f"s2#n={n}"):
            for q in (2, 6):
                for i in triple(n):
                    self.wait(i, q)
                    self.send(i, q, 2)

    def s3(self, n):
        with jax.named_scope(f"s3#n={n}"):
            for q in (1, 5, 3, 7):
                for i in triple(n):
                    self.wait(i, q)

    def drain(self, first, last):
        for i in range(first, last):
            arrived(self.w.at[i, pl.ds(0, 7 * R)], self.ssem.at[i])


class Reduce:
    def __init__(self, at, acc, near, sbuf, ibuf, obuf, outs, ssem, rsem, osem, psem, qsem, credit):
        self.at, self.acc, self.near, self.sbuf, self.ibuf, self.obuf, self.outs = at, acc, near, sbuf, ibuf, obuf, outs
        self.ssem, self.rsem, self.osem, self.psem, self.qsem, self.credit = ssem, rsem, osem, psem, qsem, credit

    def _send(self, m, s, u):
        @pl.when(u > 0)
        def _():
            pl.semaphore_wait(self.credit.at[m, s], 1)

        remote(self.sbuf[s].at[m], self.ibuf[s].at[m], self.ssem.at[m, s], self.rsem.at[m, s], self.at.neighbour((m + s) % 3)).start()

    def _sent(self, m, s, u):
        @pl.when(u > 0)
        def _():
            arrived(self.sbuf[s].at[m], self.ssem.at[m, s])

    def _taken(self, m, s, u):
        @pl.when(u < U - 1)
        def _():
            pl.semaphore_signal(self.credit.at[m, s], inc=1, device_id=self.at.neighbour((m + s) % 3), device_id_type=MESH)

    def step0(self, u):
        for m in range(M):
            self._sent(m, 0, u)
            for q in range(4, 8):
                self.sbuf[0][m, pl.ds((q - 4) * R, R), :] = self.acc[m, self.at.rows(q, m), :].astype(BF)
            self._send(m, 0, u)
        for m in range(M):
            for q in range(4):
                self.near[0][m, pl.ds(q * R, R), :] = self.acc[m, self.at.rows(q, m), :]

    def step1(self, u):
        for m in range(M):
            self._sent(m, 1, u)
            arrived(self.ibuf[0].at[m], self.rsem.at[m, 0])
            far, keep = pl.ds(2 * R, 2 * R), pl.ds(0, 2 * R)
            self.sbuf[1][m] = (self.near[0][m, far, :] + self.ibuf[0][m, far, :].astype(F32)).astype(BF)
            self._send(m, 1, u)
            self.near[1][m] = self.near[0][m, keep, :] + self.ibuf[0][m, keep, :].astype(F32)
            self._taken(m, 0, u)

    def step2(self, u):
        for m in range(M):
            self._sent(m, 2, u)
            arrived(self.ibuf[1].at[m], self.rsem.at[m, 1])
            far, keep = pl.ds(R, R), pl.ds(0, R)
            self.sbuf[2][m] = (self.near[1][m, far, :] + self.ibuf[1][m, far, :].astype(F32)).astype(BF)
            self._send(m, 2, u)
            self.near[1][m, keep, :] = self.near[1][m, keep, :] + self.ibuf[1][m, keep, :].astype(F32)
            self._taken(m, 1, u)

    def _halves(self, m):
        half = R // 2
        return [self.obuf.at[m, pl.ds(pl.multiple_of(v * half, half), half)] for v in (self.at.c, 1 - self.at.c)]

    def _out(self, m, u):
        if m == 2:
            copy(self.obuf.at[2], self.outs[2].at[u], self.osem.at[2]).start()
            return
        mine, other = self._halves(m)

        def put(p):
            block, there = pl.ds(pl.multiple_of(p * R, R), R), self.outs[m].at[:, lanes(p, self.at.c, u)]
            copy(mine.at[:, block], there, self.osem.at[m]).start()
            remote(other.at[:, block], there, self.psem.at[m], self.qsem.at[m, u], self.at.partner).start()

        each(8, put)

    def _out_done(self, m):
        if m == 2:
            arrived(self.obuf.at[2], self.osem.at[2])
            return
        mine, other = self._halves(m)
        arrived(mine, self.osem.at[m])
        arrived(other, self.psem.at[m])

    def step3(self, u):
        for m in range(M):
            @pl.when(u > 0)
            def _(m=m):
                self._out_done(m)

            arrived(self.ibuf[2].at[m], self.rsem.at[m, 2])
            self.obuf[m] = (self.near[1][m, pl.ds(0, R), :] + self.ibuf[2][m].astype(F32)).astype(BF)
            self._taken(m, 2, u)
            self._out(m, u)

    def freed(self):
        for m in range(M):
            arrived(self.sbuf[0].at[m], self.ssem.at[m, 0])

    def drain(self):
        for m in range(M):
            self._out_done(m)
            for s in (1, 2):
                arrived(self.sbuf[s].at[m], self.ssem.at[m, s])
        for m in range(2):
            for u in range(U):
                arrived(self._halves(m)[0], self.qsem.at[m, u])


def gradients(gate, up, dhid):
    dhid = dhid.astype(BF).astype(F32)
    sig = jax.nn.sigmoid(gate)
    silu = gate * sig
    return (dhid * up * (sig + silu * (1 - sig))).astype(BF), (dhid * silu).astype(BF), silu


def back_chunks(red, acc, wbuf, slot_of, ta, td, kept, tg, load, isem, hbm_out, osem, parts, hid, ticks):
    last = U * BT
    ins = (ta, td, *(kept or ()))

    def place(it):
        return it // BT, lax.rem(it, BT)

    def stores(it, s):
        u, t = place(it)
        return [copy(tg[n].at[s], hbm_out.at[n, u, tile(t, TB)], osem.at[n, s]) for n in range(2)]

    load(0, 0, 0)

    def body(it, carry):
        (u, t), s = place(it), odd(it)
        with jax.named_scope("b_wait"):
            for n, ref in enumerate(ins):
                arrived(ref.at[s], isem.at[n, s])
            for when, group in ticks.items():
                @pl.when(t == when)
                def _(group=group):
                    for tick in group:
                        tick(u)

            @pl.when(it > 1)
            def _():
                for store in stores(it - 2, s):
                    store.wait()

            load(*place(lax.rem(it + 1, last)), 1 - s)
        base = slot_of(u)

        def front(k):
            c = cols(k)
            dhid = dot(td[s], wbuf[base if kept else base + 2, c, :], NTR)
            if kept:
                gate, up = kept[0][s, :, c], kept[1][s, :, c]
            else:
                gate, up = dot(ta[s], wbuf[base, :, c], NN), dot(ta[s], wbuf[base + 1, :, c], NN)
            tg[0][s, :, c], tg[1][s, :, c], silu = gradients(gate, up, dhid)
            hid[:, c] = (silu * up).astype(BF)

        def add(m, r, c, term):
            acc[m, r, c] = jnp.where(t == 0, 0.0, acc[m, r, c]) + term

        def back(k):
            c, every = cols(k, parts), slice(None)
            for n in range(2):
                add(n, every, c, dot(ta[s], tg[n][s, :, c], TN))
            add(2, c, every, dot(hid[:, c], td[s], TN))

        with jax.named_scope("b_mm"):
            per = 4 // parts
            for k in range(4):
                front(k)
                if k >= per and k % per == 0:
                    back(k // per - 1)
            back(parts - 1)
        for store in stores(it, s):
            store.start()

        @pl.when(t == BT - 1)
        def _():
            with jax.named_scope("step0"):
                red.step0(u)

        return carry

    lax.fori_loop(0, last, body, 0)
    for n, ref in enumerate(ins):
        arrived(ref.at[last % 2], isem.at[n, last % 2])
    for it in (last - 2, last - 1):
        for store in stores(it, it % 2):
            store.wait()


def da_tiles(ta, td, tg, sb):
    def of(b, s):
        if b < 4:
            return (ta, td)[b // 2].at[s, tile(b % 2)]
        return tg[b - 4].at[0, tile(s)] if b < 6 else sb.at[b - 6, tile(s)]

    return of


def landing(acc, t):
    per = D // TT
    return acc.at[t // per, tile(lax.rem(t, per))]


def back_to_h(at, acc, wbuf, gslots, uslots, tiles, hbm_in, ksem, fbuf, fsem, lsem, h_in, dh_in, esem, results, red, ticks):
    def loads(i, s):
        row = lax.rem(i + HT, NT)
        return [copy(hbm_in.at[b % 2, b // 2, tile(row)], tiles(b, s), ksem.at[s, b]) for b in range(2 * U)]

    def eloads(t, s):
        return [copy(src.at[tile(t)], tiles(2 * U + n, s), esem.at[n, s]) for n, src in enumerate((h_in, dh_in))]

    def fsend(t, s):
        return remote(fbuf(s), landing(acc, t), fsem.at[s], lsem.at[t], at.partner)

    def results_done(t, s):
        local, *far = results(t, s)
        local.wait()
        for out in far:
            out.wait_send()

    for ld in loads(0, 0):
        ld.start()

    def body(i, carry):
        s, t = odd(i), i - HT
        for when, tick in ticks:
            pl.when(i == when)(tick)

        @pl.when((i > 1) & (i < HT + 2))
        def _():
            fsend(i - 2, s).wait_send()

        @pl.when(i == HT)
        def _():
            red.freed()
            for ld in eloads(0, 0):
                ld.start()

        for ld in loads(i, s):
            ld.wait()
        for ld in loads(lax.rem(i + 1, NT), 1 - s):
            ld.start()
        into = fbuf(s)
        for k in range(4):
            c = cols(k)
            terms = [dot(tiles(b, s)[...], wbuf[(gslots, uslots)[b % 2][b // 2], c, :], NTR) for b in range(2 * U)]
            into[:, c] = functools.reduce(jnp.add, terms)

        @pl.when(i < HT)
        def _():
            fsend(i, s).start()

        @pl.when(i >= HT)
        def _():
            for ld in eloads(t, s):
                ld.wait()
            land = landing(acc, t)
            arrived(land, lsem.at[t])
            da = into[...] + land[...]
            wide = tiles(2 * U, s)[...].astype(F32)
            scale = scale_of(wide)
            inner = jnp.mean(wide * da, -1, keepdims=True)
            dh = tiles(2 * U + 1, s)[...].astype(F32) + (scale * da - wide * (scale**3 * inner))
            tiles(2 * U, s)[...] = dh.astype(BF)
            for out in results(t, s):
                out.start()

            @pl.when(t > 0)
            def _():
                results_done(t - 1, 1 - s)

            @pl.when(t + 1 < HT)
            def _():
                for ld in eloads(t + 1, 1 - s):
                    ld.start()

        return carry

    with jax.named_scope("back_to_h"):
        lax.fori_loop(0, NT, body, 0)
    for ld in loads(0, 0):
        ld.wait()
    results_done(HT - 1, (HT - 1) % 2)


def fetcher(w, wbuf, wsem):
    def fetch(keys, slots):
        for key, slot in zip(keys.split(), map(int, slots), strict=True):
            copy(w.at[ITEMS.index(key)], wbuf.at[slot], wsem.at[slot]).start()

    def fetched(slots):
        for slot in map(int, slots):
            arrived(wbuf.at[slot], wsem.at[slot])

    return fetch, fetched


def rs_ticks(red):
    return {1: lambda u: pl.when(u > 1)(lambda: red.step2(u - 2)), 6: lambda u: rs_middle(red, u)}


def rs_middle(red, u):
    pl.when(u > 1)(lambda: red.step3(u - 2))
    pl.when(u > 0)(lambda: red.step1(u - 1))


def joined(ticks, red):
    all_of = {t: [f] for t, f in rs_ticks(red).items()}
    for (u, t), f in ticks.items():
        all_of.setdefault(t, []).append(lambda now, u=u, f=f: pl.when(now == u)(f))
    return all_of


def rs_last(red):
    return [(2, lambda: red.step2(U - 2)), (9, lambda: red.step3(U - 2)), (9, lambda: red.step1(U - 1)), (13, lambda: red.step2(U - 1))]


def first_kernel(
    x, dy, wg, wu, wd,
    w, a0, gate, up, hid, h1, a1, dyall, dgu, dh1, og, ou, od,
    st, wbuf, acc, near0, near1, sb0, sb1, sb2, ib0, ib1, ib2, obuf, ta, td, tg0, tg1, hb,
    rs_s, rs_r, rs_o, rs_p, rs_q, credit, isem, osem, ksem, fsem, lsem, esem, free, wsem,
    g_s, g_r, st_l, st_r, own, xs, xr,
):
    at = Place()
    at.greet()
    gather = Gather(at, st, w, g_s, g_r)
    c, half = at.c, R // 2
    halves = [pl.ds(pl.multiple_of(v * half, half), half) for v in (c, 1 - c)]

    def stage(n):
        for i in triple(n):
            m, l, j = ITEMS[i][0], int(ITEMS[i][1]), int(ITEMS[i][2])
            if m == "d":
                copy(wd.at[l, pl.ds(j * R, R)], st.at[i], st_l.at[i]).start()
                continue

            def put(p, i=i, src=(wg if m == "g" else wu).at[l], j=j):
                there = st.at[i, halves[0], pl.ds(pl.multiple_of(p * R, R), R)]
                remote(src.at[:, lanes(p, 1 - c, j)], there, st_l.at[NI + i], st_r.at[i], at.partner).start()
                copy(src.at[:, lanes(p, c, j)], there, st_l.at[i]).start()

            each(8, put)

    def begin(n):
        for i in triple(n):
            if ITEMS[i][0] == "d":
                arrived(st.at[i], st_l.at[i])
            else:
                arrived(st.at[i, halves[0]], st_l.at[i])
                arrived(st.at[i, halves[1]], st_r.at[i])
            copy(st.at[i], w.at[i, at.rows(0, i % 3)], own.at[i]).start()
        gather.s0(n)

    def whole(n):
        gather.s3(n)
        for i in triple(n):
            arrived(st.at[i], own.at[i])

    fetch, fetched = fetcher(w, wbuf, wsem)

    stage(0)
    begin(0)
    for n in range(1, NI // 3):
        stage(n)
    dy_out = remote(dy, dyall.at[pl.ds(T, T)], xs.at[0], xr.at[0], at.partner)
    dy_out.start()

    def xload(t, s):
        return copy(x.at[tile(t)], tg0.at[0, tile(s)], isem.at[3, s])

    def both(t, s, buf, dst, n):
        return copy(buf, dst.at[tile(t)], osem.at[0, s]), remote(buf, dst.at[tile(t + HT)], osem.at[1, s], xr.at[n], at.partner)

    def both_done(*args):
        local, far = both(*args)
        local.wait()
        far.wait_send()

    def norm_of(s):
        return td.at[0, tile(s)]

    def dyload(t, s):
        return copy(dy.at[tile(t)], td.at[1, tile(s)], isem.at[1, s])

    def dystore(t, s):
        return copy(td.at[1, tile(s)], dyall.at[tile(t)], ksem.at[s, 1])

    xload(0, 0).start()

    def norm_tile(t, carry):
        s = odd(t)
        xload(t, s).wait()

        @pl.when(t + 1 < HT)
        def _():
            xload(t + 1, 1 - s).start()

        @pl.when(t >= 2)
        def _():
            both_done(t - 2, s, norm_of(s), a0, 1)
            dystore(t - 2, s).wait()

        pl.when(t == 4)(lambda: gather.s1(0))
        dyload(t, s).start()
        wide = tg0[0, tile(s), :].astype(F32)
        norm_of(s)[...] = (wide * scale_of(wide)).astype(BF)
        dyload(t, s).wait()
        for out in (*both(t, s, norm_of(s), a0, 1), dystore(t, s)):
            out.start()
        return carry

    with jax.named_scope("norm"):
        lax.fori_loop(0, HT, norm_tile, 0)
    for t in LAST:
        both_done(t, t % 2, norm_of(t % 2), a0, 1)
        dystore(t, t % 2).wait()
    arrived(a0.at[pl.ds(T, T)], xr.at[1])
    gather.s2(0)
    begin(1)

    def aload(t, s):
        return copy(a0.at[tile(lax.rem(t, BT), TB)], ta.at[s], isem.at[0, s])

    def stores(it, s):
        j, rows = it // BT, tile(lax.rem(it, BT), TB)
        return [
            copy(acc.at[2, tile(s, TB)], gate.at[j, rows], osem.at[0, s]),
            copy(near0.at[s], up.at[j, rows], osem.at[1, s]),
            copy(td.at[s], hid.at[j, rows], ksem.at[s, 0]),
        ]

    def second():
        gather.s2(1)
        begin(2)
        whole(1)
        fetch("g01 u01 g02 u02", "2345")
        fetched("23")

    def third():
        gather.s2(2)
        begin(3)

    ticks = {3: lambda: gather.s1(1), BT: second, 12: lambda: gather.s1(2), 2 * BT: lambda: fetched("45"), 18: third}

    def gate_up(it, carry):
        j, s = it // BT, odd(it)
        aload(it, s).wait()
        for when, tick in ticks.items():
            pl.when(it == when)(tick)

        @pl.when(it > 1)
        def _():
            for store in stores(it - 2, s):
                store.wait()

        aload(it + 1, 1 - s).start()
        for k in range(4):
            cc = cols(k)
            g, v = (dot(ta[s], wbuf[2 * j + n, :, cc], NN) for n in range(2))
            acc[2, tile(s, TB), cc] = g
            near0[s, :, cc] = v
            td[s, :, cc] = (jax.nn.silu(g) * v).astype(BF)
        for store in stores(it, s):
            store.start()
        return carry

    aload(0, 0).start()
    whole(0)
    fetch("g00 u00", "01")
    fetched("01")
    with jax.named_scope("gate_up"):
        lax.fori_loop(0, U * BT, gate_up, 0)
    aload(0, 0).wait()
    for it in range(2):
        for store in stores(U * BT - 2 + it, it):
            store.wait()

    def hloads(i, s):
        row = lax.rem(i + HT, NT)
        return [copy(hid.at[j, tile(row)], sb0.at[j, tile(s)], isem.at[j, s]) for j in range(U)]

    def sums(s):
        return acc.at[2, tile(s)]

    def fsend(t, s):
        return remote(sums(s), landing(acc, t), fsem.at[s], lsem.at[t], at.partner)

    for ld in hloads(0, 0):
        ld.start()
    whole(2)
    fetch("d00 d01 d02", "012")
    fetched("012")
    gather.s1(3)
    xload(0, 0).start()

    def down(i, s):
        for ld in hloads(i, s):
            ld.wait()

        @pl.when(i + 1 < NT)
        def _():
            for ld in hloads(i + 1, 1 - s):
                ld.start()

        for k in range(4):
            cc = cols(k)
            terms = [dot(sb0[j, tile(s), :], wbuf[j, :, cc], NN) for j in range(U)]
            sums(s)[:, cc] = functools.reduce(jnp.add, terms)

    def hout(t, s):
        return copy(td.at[1, tile(s)], h1.at[tile(t)], ksem.at[s, 0])

    def down_tile(i, carry):
        s = odd(i)

        @pl.when((i > 1) & (i < HT + 2))
        def _():
            fsend(i - 2, s).wait_send()

        @pl.when(i == HT + 1)
        def _():
            gather.s2(3)
            begin(4)

        down(i, s)

        @pl.when(i < HT)
        def _():
            fsend(i, s).start()

        @pl.when(i >= HT)
        def _():
            t = i - HT
            xload(t, s).wait()

            @pl.when(t + 1 < HT)
            def _():
                xload(t + 1, 1 - s).start()

            @pl.when(t > 1)
            def _():
                both_done(t - 2, s, norm_of(s), a1, 2)
                hout(t - 2, s).wait()

            land = landing(acc, t)
            arrived(land, lsem.at[t])
            h = tg0[0, tile(s), :] + (sums(s)[...] + land[...]).astype(BF)
            td[1, tile(s), :] = h
            wide = h.astype(F32)
            norm_of(s)[...] = (wide * scale_of(wide)).astype(BF)
            for out in (*both(t, s, norm_of(s), a1, 2), hout(t, s)):
                out.start()

        return carry

    with jax.named_scope("down"):
        lax.fori_loop(0, NT, down_tile, 0)
    for t in LAST:
        both_done(t, t % 2, norm_of(t % 2), a1, 2)
        hout(t, t % 2).wait()
    whole(3)
    fetch("g10 u10 d10", "345")
    arrived(dyall.at[pl.ds(T, T)], xr.at[0])
    dy_out.wait_send()
    arrived(a1.at[pl.ds(T, T)], xr.at[2])
    fetched("345")

    red = Reduce(at, acc, (near0, near1), (sb0, sb1, sb2), (ib0, ib1, ib2), obuf, (og, ou, od), rs_s, rs_r, rs_o, rs_p, rs_q, credit)

    def fifth():
        gather.s2(4)
        begin(5)

    def weights1():
        whole(4)
        fetch("g11 u11 d11", "012")

    def weights2():
        whole(5)
        fetch("g12 u12 d12", "345")

    ticks = {
        (0, 1): lambda: gather.s1(4),
        (0, 3): fifth,
        (0, 6): weights1,
        (0, 7): lambda: gather.s1(5),
        (1, 0): lambda: fetched("012"),
        (1, 2): lambda: gather.s2(5),
        (1, 6): weights2,
        (2, 0): lambda: fetched("345"),
        (2, 1): lambda: fetch("g10 u10 g11", "012"),
    }

    def load(u, t, s):
        for n, (src, dst) in enumerate(((a1, ta), (dyall, td))):
            copy(src.at[tile(t, TB)], dst.at[s], isem.at[n, s]).start()

    back_chunks(red, acc, wbuf, lambda u: 3 * odd(u + 1), ta, td, None, (tg0, tg1), load, isem, dgu, osem, 4, hb, joined(ticks, red))
    pl.semaphore_signal(free, inc=1, device_id=at.partner, device_id_type=MESH)
    fetch("u11", "5")
    fetched("0125")
    pl.semaphore_wait(free, 1)

    tiles = da_tiles(ta, td, (tg0, tg1), sb0)

    def results(t, s):
        return both(t, s, tiles(2 * U, s), dh1, 3)

    back_to_h(at, acc, wbuf, (0, 2, 3), (1, 5, 4), tiles, dgu, ksem, sums, fsem, lsem, h1, dy, esem, results, red, rs_last(red))
    with jax.named_scope("tail"):
        red.step3(U - 1)
        arrived(dh1.at[pl.ds(T, T)], xr.at[3])
        gather.drain(0, NI)
        for i, item in enumerate(ITEMS):
            if item[0] != "d":
                arrived(st.at[i, halves[0]], st_l.at[NI + i])
        red.drain()


def second_kernel(
    x, w, a0, gate, up, dh,
    dx, dgu, og, ou, od,
    wbuf, acc, near0, near1, sb0, sb1, sb2, ib0, ib1, ib2, obuf, ta, td, tg0, tg1, hb,
    rs_s, rs_r, rs_o, rs_p, rs_q, credit, isem, osem, ksem, fsem, lsem, esem, free, wsem,
    gt0, gt1,
):
    at = Place()

    fetch, fetched = fetcher(w, wbuf, wsem)

    fetch("d00", "0")
    at.greet()
    red = Reduce(at, acc, (near0, near1), (sb0, sb1, sb2), (ib0, ib1, ib2), obuf, (og, ou, od), rs_s, rs_r, rs_o, rs_p, rs_q, credit)

    def load(u, t, s):
        for n, (src, dst) in enumerate(((a0, ta), (dh, td), (gate.at[u], gt0), (up.at[u], gt1))):
            copy(src.at[tile(t, TB)], dst.at[s], isem.at[n, s]).start()

    ticks = {
        (0, 0): lambda: fetched("0"),
        (0, 1): lambda: fetch("d01 d02", "12"),
        (0, 3): lambda: fetch("g00 u00 g01", "345"),
        (0, 7): lambda: fetched("12"),
        (1, 1): lambda: fetch("u01", "0"),
        (2, 1): lambda: fetch("g02", "1"),
    }
    back_chunks(red, acc, wbuf, lambda u: u, ta, td, (gt0, gt1), (tg0, tg1), load, isem, dgu, osem, 2, hb, joined(ticks, red))
    pl.semaphore_signal(free, inc=1, device_id=at.partner, device_id_type=MESH)
    fetch("u02", "2")
    fetched("345012")
    pl.semaphore_wait(free, 1)

    tiles = da_tiles(ta, td, (tg0, tg1), sb0)

    def results(t, s):
        return [copy(tiles(2 * U, s), dx.at[tile(t)], osem.at[0, s])]

    back_to_h(at, acc, wbuf, (3, 5, 1), (4, 0, 2), tiles, dgu, ksem, lambda s: gt0.at[s, pl.ds(0, TT)], fsem, lsem, x, dh, esem, results, red, rs_last(red))
    with jax.named_scope("tail"):
        red.step3(U - 1)
        red.drain()


def solution(mesh):
    f32, bf = (lambda *s: jax.ShapeDtypeStruct(s, F32)), (lambda *s: jax.ShapeDtypeStruct(s, BF))
    dma, regular = pltpu.SemaphoreType.DMA, pltpu.SemaphoreType.REGULAR
    grads = [bf(R // 2, 2 * U * CW), bf(R // 2, 2 * U * CW), bf(U, R, D)]
    spread = [(3, 4 * R, D), (3, 2 * R, D), (3, R, D)]
    shared = [
        pltpu.VMEM((6, D, CW), BF),
        pltpu.VMEM((3, D, D), F32),
        *(pltpu.VMEM(s, F32) for s in spread[:2]),
        *(pltpu.VMEM(s, BF) for s in spread),
        *(pltpu.VMEM(s, BF) for s in spread),
        pltpu.VMEM((3, R, D), BF),
        *[pltpu.VMEM((2, TB, D), BF)] * 4,
        pltpu.VMEM((TB, CW), BF),
        dma((3, 3)), dma((3, 3)), dma((3,)), dma((2,)), dma((2, U)), regular((3, 3)),
        dma((4, 2)), dma((2, 2)), dma((2, 6)), dma((2,)), dma((HT,)), dma((2, 2)), regular, dma((6,)),
    ]

    def call(kernel, number, outs, scratch, *args):
        anywhere = pl.BlockSpec(memory_space=pl.ANY)
        return pl.pallas_call(
            kernel,
            out_shape=outs,
            in_specs=[anywhere] * len(args),
            out_specs=[anywhere] * len(outs),
            scratch_shapes=scratch,
            compiler_params=pltpu.CompilerParams(collective_id=number, has_side_effects=True, vmem_limit_bytes=VMEM_LIMIT),
        )(*args)

    def body(x, dy, w_gate, w_up, w_down):
        x, dy = x[0], dy[0]

        hidden = [f32(U, 2 * T, CW), f32(U, 2 * T, CW), bf(U, 2 * T, CW)]
        dgu = bf(2, U, 2 * T, CW)
        w, a0, gate, up, _, _, _, _, _, dh, *g1 = call(
            first_kernel, 0,
            [bf(NI, D, CW), bf(2 * T, D), *hidden, bf(T, D), *[bf(2 * T, D)] * 2, dgu, bf(2 * T, D), *grads],
            [
                pltpu.VMEM((NI, R, CW), BF), *shared,
                dma((NI,)), dma((NI, 7)), dma((2 * NI,)), dma((NI,)), dma((NI,)), dma((1,)), dma((4,)),
            ],
            x, dy, w_gate, w_up, w_down,
        )
        dx, _, *g0 = call(
            second_kernel, 1,
            [bf(T, D), dgu, *grads],
            [*shared, *[pltpu.VMEM((2, TB, CW), F32)] * 2],
            x, w, a0, gate, up, dh,
        )
        downs = jnp.stack([g0[2], g1[2]]).reshape(2, U * R, D)
        return dx[None], jnp.stack([g0[0], g1[0]]), jnp.stack([g0[1], g1[1]]), downs

    rows, data = P(None, "dp", None), P(("rep", "dp"), None, None)
    return jax.shard_map(body, mesh=mesh, in_specs=(data, data, rows, rows, rows), out_specs=(data, rows, rows, rows), check_vma=False)
```
